32 devices in a mesh: grp: 4 (over y, x), sub: 8 (over z, core).
Axes of the slice: x: 2, y: 2, z: 4, core: 2. Of those that a mesh axis runs over, the one named last changes fastest.
Arguments:
- bem_tiles: float32 [4096, 4096], P('grp', 'sub'), may hold values from -0.0625 to 0.0625
- leaf_inverse: float32 [4, 16, 1024, 1024], P('grp', 'sub'), may hold values from -1.5 to 1.5
- coupling: float32 [4, 16, 1024, 512], P('grp', 'sub'), may hold values from -0.0625 to 0.0625
- schur_inverse: float32 [4, 512, 512], P('grp', None, 'sub'), may hold values from -1.5 to 1.5
- leaf_load: float32 [4, 16, 1024, 128], P('grp', 'sub'), may hold values from -6 to 6
- sep_load: float32 [4, 512, 128], P('grp'), may hold values from -6 to 6
- surf_load: float32 [4096, 128], P(('grp', 'sub')), may hold values from -6 to 6
- surf_start: float32 [4096, 128], P(('grp', 'sub')), may hold values from -6 to 6
- flux_weight: float32 [4, 16, 8, 128], P('grp', 'sub'), may hold values from 0.25 to 1
- trace_weight: float32 [4, 16, 8, 128], P('grp', 'sub'), may hold values from 0.25 to 1
- leaf_sizes: int32 [4, 16], P('grp', 'sub'), may hold values from 512 to 1024
- block_counts: int32 [4, 16], P('grp', 'sub'), may hold values from 4 to 8
- block_owner: int32 [4, 16, 8, 1], P('grp', 'sub'), may hold values from 0 to 7; in each aligned block of 16 rows (0 to 15, 16 to 31, ..., all dimensions but the last counted through in order) at most 2 rows name the same one
Outputs:
- solution: float32 [4, 16, 1024, 128], P('grp', 'sub')
- sep_value: float32 [4, 512, 128], P('grp', 'sub')
- pressure: float32 [4096, 128], P(('grp', 'sub'))
The draws below stay inside these ranges and needn't reach their ends.
Inputs may be any that keep to these rules, and one draw needn't show every extreme that they name: `block_owner`: of the 16 entries of one device, live or not, at most 2 name the same owner, and some device has 2 entries naming one owner.
All inputs are finite; a program needn't handle non-finite values.
Results may differ from the reference program's by a relative error of at most 0.00018.
Values sent between devices are 32-bit elements; how exact they have to be, the bound alone decides.
A program may use at most 128 MiB of HBM per device.

```python
import math
import jax
import jax.numpy as jnp
import numpy as np
from jax import lax

LEAF = 1024
SEP = 512
SURF_DEV = 128
SUB_DEV = 2
CAP = 2
SWEEPS = 3
LOADS = 128
GROUPS = 4
NSUBD = 16
NS = 4096
MAXB = 8
N_SUB = 8


def draw_leaf_inverse(key, part):
    first, second = jax.random.split(jax.random.fold_in(key, 11))
    spread = jax.random.normal(first, (GROUPS, NSUBD, LEAF, LEAF), jnp.float32) * (0.3 / math.sqrt(LEAF))
    diagonal = jax.random.uniform(second, (GROUPS, NSUBD, LEAF), jnp.float32, 0.4, 0.7)
    return spread + diagonal[..., None] * jnp.eye(LEAF, dtype=jnp.float32)


def draw_schur_inverse(key, part):
    first, second = jax.random.split(jax.random.fold_in(key, 23))
    spread = jax.random.normal(first, (GROUPS, SEP, SEP), jnp.float32) * (0.3 / math.sqrt(SEP))
    diagonal = jax.random.uniform(second, (GROUPS, SEP), jnp.float32, 0.4, 0.7)
    return spread + diagonal[..., None] * jnp.eye(SEP, dtype=jnp.float32)


def with_ends(result, own_key, low, largest):
    index_at = [jax.random.randint(jax.random.fold_in(own_key, axis), (), 0, length) for axis, length in enumerate(result.shape)]
    longest = result.shape.index(max(result.shape))
    beside = index_at[:longest] + [(index_at[longest] + 1) % result.shape[longest]] + index_at[longest + 1:]
    return result.at[tuple(index_at)].set(low).at[tuple(beside)].set(largest)


def spiked(array, rng, source, target, parts, factor):
    owner, partner = [(jnp.arange(array.shape[axis_at]) // (array.shape[axis_at] // parts)).reshape([-1 if axis == axis_at else 1 for axis in range(array.ndim)]) for axis_at in (source, target)]
    chosen = jax.random.permutation(rng, parts)[partner]
    strong = (owner == chosen) | (owner == (partner + parts // 2) % parts)
    return jnp.where(strong, factor * array, array)


def block_levels(own_key, dims, pieces, least, top_value):
    level = 1.0
    for axis_at, blocks in pieces:
        steps = jax.random.uniform(jax.random.fold_in(jax.random.fold_in(own_key, 6), axis_at), (blocks,), jnp.float32, least / len(pieces), top_value / len(pieces))
        level = level * jnp.repeat(jnp.exp(steps), dims[axis_at] // blocks).reshape((-1,) + (1,) * (len(dims) - 1 - axis_at))
    return level


def deal_out(own_key, own, number, rows, count, top, reach, lean):
    ranking = jax.random.permutation(own_key, count)
    crowded, usual = load_shares(count, rows * top, reach, lean, True), load_shares(count, rows * top, reach, lean, False)
    places = jnp.arange(count)

    def named(lengths, turn):
        used = int((lengths > 0).sum())
        fixed = max(1, used // 4)
        shifted = fixed + (places - fixed + turn * (used - fixed)) % max(1, count - fixed)
        return jnp.zeros((count,), jnp.int32).at[ranking[jnp.where(places < fixed, places, shifted)]].set(jnp.asarray(lengths, jnp.int32))

    lengths = jnp.where(number % 4 == 0, named(crowded, number // 4), named(usual, number - number // 4 - 1))
    mixed = jax.random.permutation(jax.random.fold_in(own, 3), count)
    source_of, taker = mixed[0:count // 2 * 2:2], mixed[1:count // 2 * 2:2]
    margin = jnp.minimum(lengths[source_of] - 1, reach - lengths[taker]) // 2
    margin = jnp.where((source_of == ranking[0]) | (taker == ranking[0]) | (lengths[taker] == 0), 0, jnp.maximum(margin, 0))
    shifted = jax.random.randint(jax.random.fold_in(own, 4), (count // 2,), 0, 1 << 20) % (margin + 1)
    lengths = lengths.at[source_of].add(-shifted).at[taker].add(shifted)
    items = jnp.searchsorted(jnp.cumsum(lengths), jnp.arange(rows * top), side="right").astype(jnp.int32)
    listing = items.reshape(top, rows).T
    listing = listing[jax.random.permutation(jax.random.fold_in(own, 1), rows)]
    turn = jax.random.randint(jax.random.fold_in(own, 2), (rows, 1), 0, top)
    return jnp.take_along_axis(listing, (jnp.arange(top)[None, :] + turn) % top, axis=1)


def load_shares(number_of, total, reach, skew, full):
    portions = [(1 << 20) // math.isqrt(grade ** skew) + 1 for grade in range(1, number_of + 1)]
    largest = reach if full else min(reach, max(-(-total // number_of), total * portions[0] // sum(portions)))
    least = 1 if total - largest >= number_of - 1 else 0
    given, surplus = [largest] + [least] * (number_of - 1), total - largest - least * (number_of - 1)
    while surplus > 0:
        movable = [i for i in range(1, number_of) if given[i] < largest] or [i for i in range(1, number_of) if given[i] < reach]
        mass, budget = sum([portions[i] for i in movable]), surplus
        for i in movable:
            addition = min(reach - given[i], max(1, budget * portions[i] // mass), surplus)
            given[i] = given[i] + addition
            surplus = surplus - addition
    return np.array(given)


def gaussian(own_key, shape, deviation, limit, cuts=(), held_as=jnp.bfloat16):
    array = deviation * jax.random.normal(own_key, shape, jnp.float32)
    if cuts:
        array = array * block_levels(own_key, shape, cuts, -0.22, 0.18)
    return jnp.clip(array, -limit, limit).astype(held_as)


def heavy_noise(own_key, shape, scale, bound, cuts, heavy, kind=jnp.bfloat16):
    result = scale * jax.random.normal(own_key, shape, jnp.float32)
    if cuts:
        result = result * block_levels(own_key, shape, cuts, -0.22, 0.18)
    return jnp.clip(spiked(result, jax.random.fold_in(own_key, 3), *heavy), -bound, bound).astype(kind)


def setup_inputs(seed: int = 0) -> dict:
    key_of = jax.random.split(jax.random.key(seed), 14)
    bem_tiles = heavy_noise(key_of[0], (NS, NS), (4 * NS) ** -0.5, 0.0625, ((0, 4), (1, 8)), (1, 0, 8, 2.0), jnp.float32)
    leaf_inverse = draw_leaf_inverse(jax.random.fold_in(key_of[13], 71), 0)
    coupling = gaussian(key_of[2], (GROUPS, NSUBD, LEAF, SEP), (8 * LEAF) ** -0.5, 0.0625, ((0, 4), (1, 8)), jnp.float32)
    schur_inverse = draw_schur_inverse(jax.random.fold_in(key_of[13], 71), 0)
    leaf_load = gaussian(key_of[4], (GROUPS, NSUBD, LEAF, LOADS), 1.0, 6.0, ((0, 4), (1, 8)), jnp.float32)
    sep_load = gaussian(key_of[5], (GROUPS, SEP, LOADS), 1.0, 6.0, ((0, 4),), jnp.float32)
    surf_load = gaussian(key_of[6], (NS, LOADS), 1.0, 6.0, ((0, 32),), jnp.float32)
    surf_start = gaussian(key_of[7], (NS, LOADS), 1.0, 6.0, ((0, 32),), jnp.float32)
    flux_weight = jnp.clip(jnp.exp(math.log(1.0) - 1.3862944 * jax.random.uniform(key_of[8], (GROUPS, NSUBD, MAXB, SURF_DEV), jnp.float32) ** block_levels(key_of[8], (GROUPS, NSUBD, MAXB, SURF_DEV), ((0, 4), (1, 8)), -0.2, 0.2)), 0.25, 1.0)
    trace_weight = jnp.clip(jnp.exp(math.log(1.0) - 1.3862944 * jax.random.uniform(key_of[9], (GROUPS, NSUBD, MAXB, SURF_DEV), jnp.float32) ** block_levels(key_of[9], (GROUPS, NSUBD, MAXB, SURF_DEV), ((0, 4), (1, 8)), -0.2, 0.2)), 0.25, 1.0)
    leaf_sizes = with_ends(jax.random.randint(key_of[10], (GROUPS, NSUBD), LEAF // 2, LEAF + 1), jax.random.fold_in(key_of[10], 1), LEAF // 2, LEAF).astype(jnp.int32)
    block_counts = with_ends(jax.random.randint(key_of[11], (GROUPS, NSUBD), MAXB // 2, MAXB + 1), jax.random.fold_in(key_of[11], 1), MAXB // 2, MAXB).astype(jnp.int32)
    block_owner_keys = jax.random.split(jax.random.fold_in(key_of[12], 1), GROUPS * NSUBD * MAXB // (SUB_DEV * MAXB))
    block_owner_turns = jax.random.permutation(jax.random.fold_in(key_of[12], 3), GROUPS * NSUBD * MAXB // (SUB_DEV * MAXB))
    block_owner = jax.vmap(lambda own, number: deal_out(jax.random.fold_in(key_of[12], 2), own, number, SUB_DEV * MAXB, N_SUB, 1, CAP, 2))(block_owner_keys, block_owner_turns).reshape((GROUPS, NSUBD, MAXB, 1))
    return {"bem_tiles": bem_tiles, "leaf_inverse": leaf_inverse, "coupling": coupling, "schur_inverse": schur_inverse, "leaf_load": leaf_load, "sep_load": sep_load, "surf_load": surf_load, "surf_start": surf_start, "flux_weight": flux_weight, "trace_weight": trace_weight, "leaf_sizes": leaf_sizes, "block_counts": block_counts, "block_owner": block_owner}


def reference(bem_tiles, leaf_inverse, coupling, schur_inverse, leaf_load, sep_load, surf_load, surf_start, flux_weight, trace_weight, leaf_sizes, block_counts, block_owner):
    highest = lax.Precision.HIGHEST
    mask = (jnp.arange(LEAF, dtype=jnp.int32)[None, None, :] < leaf_sizes[:, :, None]).astype(jnp.float32)
    active = (jnp.arange(MAXB, dtype=jnp.int32)[None, None, :] < block_counts[:, :, None]).astype(jnp.float32)
    picker = (block_owner[..., 0][..., None] == jnp.arange(N_SUB, dtype=jnp.int32)[None, None, None, :]).astype(jnp.float32)
    live_pick = picker * active[..., None]
    trace_scale = trace_weight * active[..., None]
    pressure = surf_start
    sep_value = jnp.zeros((GROUPS, SEP, LOADS), jnp.float32)
    solution = jnp.zeros((GROUPS, NSUBD, LEAF, LOADS), jnp.float32)
    for sweep in range(SWEEPS):
        blocks_surface = pressure.reshape(GROUPS, N_SUB, SURF_DEV, LOADS)
        tiled = jnp.transpose(blocks_surface, (1, 0, 2, 3)).reshape(NS, LOADS)
        applied = jnp.dot(bem_tiles, tiled, precision=highest, preferred_element_type=jnp.float32)
        flux = jnp.einsum("gjko,goil->gjkil", live_pick, blocks_surface, precision=highest) * flux_weight[..., None]
        flux = flux.reshape(GROUPS, NSUBD, LEAF, LOADS)
        pulled = jnp.einsum("gjrs,gsl->gjrl", coupling, sep_value, precision=highest)
        rhs = (leaf_load - pulled - flux) * mask[..., None]
        solution = jnp.einsum("gjrc,gjcl->gjrl", leaf_inverse, rhs, precision=highest) * mask[..., None]
        total = jnp.einsum("gjrs,gjrl->gsl", coupling, solution, precision=highest)
        sep_value = jnp.einsum("gst,gtl->gsl", schur_inverse, sep_load - total, precision=highest)
        weighted = solution.reshape(GROUPS, NSUBD, MAXB, SURF_DEV, LOADS) * trace_scale[..., None]
        trace = jnp.einsum("gjko,gjkil->goil", picker, weighted, precision=highest).reshape(NS, LOADS)
        pressure = surf_load + applied + trace
    return solution, sep_value, pressure
```

```python
import jax
import jax.numpy as jnp
from jax import lax
from jax.sharding import PartitionSpec as P

CAP = 2
SWEEPS = 3


def on_device(
    bem_tiles,
    leaf_inverse,
    coupling,
    schur_inverse,
    leaf_load,
    sep_load,
    surf_load,
    surf_start,
    flux_weight,
    trace_weight,
    leaf_sizes,
    block_counts,
    block_owner,
):
    highest = lax.Precision.HIGH
    parts = lax.axis_size("sub")
    here = lax.axis_index("sub")
    width = surf_load.shape[0]
    loads = surf_load.shape[1]
    leaves = leaf_inverse.shape[1]
    order = leaf_inverse.shape[2]
    blocks = order // width
    entries = leaves * blocks
    separator = schur_inverse.shape[1]
    sep_share = schur_inverse.shape[2]
    row_mask = (jnp.arange(order, dtype=jnp.int32)[None, :] < leaf_sizes[0][:, None]).astype(
        jnp.float32
    )[:, :, None]
    active = (
        (jnp.arange(blocks, dtype=jnp.int32)[None, :] < block_counts[0][:, None])
        .astype(jnp.float32)
        .reshape(entries)
    )
    owner = block_owner[0, :, :, 0].reshape(entries)
    picker = (owner[:, None] == jnp.arange(parts, dtype=jnp.int32)[None, :]).astype(jnp.float32)
    live_pick = picker * active[:, None]
    flux_scale = flux_weight[0].reshape(entries, width)[:, :, None]
    trace_scale = (trace_weight[0].reshape(entries, width) * active[:, None])[:, :, None]
    schur_full = lax.all_gather(schur_inverse[0], "sub", axis=1, tiled=True)
    pressure = surf_start
    sep_value = jnp.zeros((separator, loads), jnp.float32)
    solution = jnp.zeros((leaves, order, loads), jnp.float32)
    for sweep in range(SWEEPS):
        column = lax.all_gather(pressure, "grp", axis=0, tiled=True)
        product = jnp.dot(bem_tiles, column, precision=highest, preferred_element_type=jnp.float32)
        surface_patch = lax.all_gather(pressure, "sub", axis=0, tiled=True).reshape(
            parts, width, loads
        )
        flux = jnp.einsum("eo,oil->eil", live_pick, surface_patch, precision=highest) * flux_scale
        flux = flux.reshape(leaves, order, loads)
        pulled = jnp.einsum("jrs,sl->jrl", coupling[0], sep_value, precision=highest)
        rhs = (leaf_load[0] - pulled - flux) * row_mask
        solution = jnp.einsum("jrc,jcl->jrl", leaf_inverse[0], rhs, precision=highest) * row_mask
        partial_sum = jnp.einsum("jrs,jrl->sl", coupling[0], solution, precision=highest)
        summed = lax.psum(partial_sum, "sub")
        sep_value = jnp.dot(
            schur_full, sep_load[0] - summed, precision=highest, preferred_element_type=jnp.float32
        )
        weighted = solution.reshape(entries, width, loads) * trace_scale
        outgoing = jnp.dot(
            picker.T,
            weighted.reshape(entries, width * loads),
            precision=highest,
            preferred_element_type=jnp.float32,
        )
        pressure = surf_load + lax.psum_scatter(
            product + outgoing.reshape(parts * width, loads), "sub", scatter_dimension=0, tiled=True
        )
    sep_rows_out = lax.dynamic_slice_in_dim(sep_value, here * sep_share, sep_share, 0)
    return (solution[None], sep_rows_out[None], pressure)


def solution(mesh):
    return jax.shard_map(
        on_device,
        mesh=mesh,
        in_specs=(
            P("grp", "sub"),
            P("grp", "sub", None, None),
            P("grp", "sub", None, None),
            P("grp", None, "sub"),
            P("grp", "sub", None, None),
            P("grp", None, None),
            P(("grp", "sub"), None),
            P(("grp", "sub"), None),
            P("grp", "sub", None, None),
            P("grp", "sub", None, None),
            P("grp", "sub"),
            P("grp", "sub"),
            P("grp", "sub", None, None),
        ),
        out_specs=(P("grp", "sub", None, None), P("grp", "sub", None), P(("grp", "sub"), None)),
        check_vma=False,
    )
```
